512 devices in a mesh: date: 64 (over z, y), pix: 8 (over x, core).
Axes of the slice: x: 4, y: 8, z: 8, core: 2. Of those that a mesh axis runs over, the one named last changes fastest.
Arguments:
- reflect: bfloat16 [64, 6, 65536], P('date', None, 'pix'), may hold values from -8 to 8
- cloud_free: int32 [64, 65536], P('date', 'pix'), may hold values from 0 to 1, as said below
- days: int32 [64], P('date'), may hold values from 1 to 2079, as said below
Outputs:
- median: float32 [6, 65536], P(None, 'pix')
- slope: float32 [6, 65536], P(None, 'pix')
The draws below stay inside these ranges and needn't reach their ends.
Inputs may be any that keep to these rules, and one draw needn't show every extreme that they name: `cloud_free`: every pixel is clear on at least one of the first 32 dates and on at least one of the others; clear shares differ between tiles. `days`: strictly increasing.
All inputs are finite; a program needn't handle non-finite values.
Results may differ from the reference program's by a relative error of at most 0.0003.
Values may be sent and summed in bfloat16 or wider, within the bound.
A program may use at most 64 MiB of HBM per device.

```python
import jax
import jax.numpy as jnp
from jax import lax

DATES = 64
BANDS = 6
PIX_DEV = 8192
PIXELS = 65536


def draw_reflect(key, part):
    keys = jax.random.split(key, 4)
    tiles = PIXELS // PIX_DEV
    region = jax.random.normal(keys[0], (1, BANDS, tiles), jnp.float32)
    haze = 0.6 * jax.random.normal(keys[1], (DATES, BANDS, 1), jnp.float32)
    tile_date = 0.5 * jax.random.normal(keys[2], (DATES, BANDS, tiles), jnp.float32)
    base = jnp.repeat(region + tile_date, PIX_DEV, axis=2) + haze
    noise = 0.8 * jax.random.normal(keys[3], (DATES, BANDS, PIXELS), jnp.float32)
    return jnp.clip(base + noise, -8.0, 8.0).astype(jnp.bfloat16)


def draw_cloud_free(key, part):
    keys = jax.random.split(key, 4)
    tiles = PIXELS // PIX_DEV
    cloudy = jnp.repeat(jax.random.randint(keys[0], (tiles,), 10, 85), PIX_DEV)
    rolls = jax.random.randint(keys[1], (DATES, PIXELS), 0, 100)
    clear = rolls >= cloudy[None, :]
    first = jax.random.randint(keys[2], (PIXELS,), 0, DATES // 2)
    second = jax.random.randint(keys[3], (PIXELS,), DATES // 2, DATES)
    rows = jnp.arange(DATES, dtype=jnp.int32)[:, None]
    clear = clear | (rows == first[None, :]) | (rows == second[None, :])
    return clear.astype(jnp.int32)


def draw_days(key, part):
    keys = jax.random.split(key, 2)
    start = jax.random.randint(keys[0], (), 0, 31)
    gaps = jax.random.randint(keys[1], (DATES,), 1, 33)
    raw = (start + jnp.cumsum(gaps)).astype(jnp.int32)
    index = jnp.arange(DATES, dtype=jnp.int32)
    raw = jnp.where(index == 0, jnp.int32(1), raw)
    raw = jnp.where(index == DATES - 1, jnp.int32(31 + 32 * DATES), raw)
    return raw.astype(jnp.int32)


def setup_inputs(seed: int = 0) -> dict:
    arg_keys = jax.random.split(jax.random.key(seed), 4)
    reflect = draw_reflect(jax.random.fold_in(arg_keys[3], 71), 0)
    cloud_free = draw_cloud_free(jax.random.fold_in(arg_keys[3], 71), 0)
    days = draw_days(jax.random.fold_in(arg_keys[3], 71), 0)
    return {"reflect": reflect, "cloud_free": cloud_free, "days": days}


ridge = 1.0


def rank_block(pair):
    xb, mb = pair
    zeros = jnp.zeros(xb.shape, jnp.float32)

    def step(i, carry):
        less, equal = carry
        xt = lax.dynamic_index_in_dim(xb, i, 0, keepdims=True)
        mt = lax.dynamic_index_in_dim(mb, i, 0, keepdims=True)[:, None, :]
        less = less + mt * (xt < xb).astype(jnp.float32)
        equal = equal + mt * (xt == xb).astype(jnp.float32)
        return (less, equal)

    less, equal = lax.fori_loop(0, xb.shape[0], step, (zeros, zeros))
    count = jnp.sum(mb, 0)
    lower = jnp.floor((count - 1.0) / 2.0)
    upper = jnp.floor(count / 2.0)

    def pick(level):
        chosen = mb[:, None, :] * ((less <= level) & (level < less + equal)).astype(jnp.float32)
        return jnp.sum(chosen * xb, 0) / jnp.maximum(jnp.sum(chosen, 0), 1.0)

    return 0.5 * (pick(lower) + pick(upper))


def reference(reflect, cloud_free, days):
    x = reflect.astype(jnp.float32)
    m = cloud_free.astype(jnp.float32)
    t = days.astype(jnp.float32) / 365.0
    csum = jnp.sum(x * m[:, None, :], 2)
    cnt = jnp.sum(m, 1)
    scene_mean = csum / jnp.maximum(cnt, 1.0)[:, None]
    y = x - scene_mean[:, :, None]
    s0 = jnp.sum(m, 0)
    s1 = jnp.sum(t[:, None] * m, 0)
    s2 = jnp.sum((t * t)[:, None] * m, 0)
    sy = jnp.sum(m[:, None, :] * y, 0)
    sty = jnp.sum((t[:, None] * m)[:, None, :] * y, 0)
    first = s0 + ridge
    det = first * (s2 + ridge) - s1 * s1
    slope = (first[None, :] * sty - s1[None, :] * sy) / det[None, :]
    blocks = PIXELS // PIX_DEV
    xs = x.reshape(DATES, BANDS, blocks, PIX_DEV).transpose(2, 0, 1, 3)
    ms = m.reshape(DATES, blocks, PIX_DEV).transpose(1, 0, 2)
    med = lax.map(rank_block, (xs, ms))
    median = med.transpose(1, 0, 2).reshape(BANDS, PIXELS)
    return median, slope
```

```python
import functools

import jax
import jax.numpy as jnp
from jax import lax
from jax.experimental import pallas as pl
from jax.experimental.pallas import tpu as pltpu
from jax.sharding import Mesh
from jax.sharding import PartitionSpec as P

MESH = pl.DeviceIdType.MESH
DATE = ("date_0", "date_1")
SIDE = 8
DATES = SIDE * SIDE
PEERS = 8
LANES = 128
TILE = 8192
HALF = SIDE // 2
WORKERS = HALF * SIDE
WIDTH = TILE // WORKERS
CHUNKS = TILE // LANES
BANDS = 6
KEPT = DATES // 2 + 1
sentinel = 100.0
per_year = 1.0 / 365.0


def merged(lo, hi, r):
    step = 2 * r
    if step < hi - lo:
        yield from merged(lo, hi, step)
        yield from merged(lo + r, hi, step)
        yield from ((i, i + r) for i in range(lo + r, hi - r, step))
    else:
        yield (lo, lo + r)


def sorted_pairs(lo, hi):
    if hi > lo:
        mid = lo + (hi - lo) // 2
        yield from sorted_pairs(lo, mid)
        yield from sorted_pairs(mid + 1, hi)
        yield from merged(lo, hi, 1)


def pruned_network(n, kept):
    needed, steps = set(range(kept)), []
    for a, b in reversed(list(sorted_pairs(0, n - 1))):
        low, high = a in needed, b in needed
        if low or high:
            steps.append((a, b, low, high))
            needed |= {a, b}
    return steps[::-1]


ORDER = sorted(range(WORKERS), key=lambda w: (w // SIDE, min(w % SIDE, SIDE - w % SIDE)))
DEAL = ORDER[::-1]
NETWORK = pruned_network(DATES, KEPT)


def place():
    return lax.axis_index("date_0"), lax.axis_index("date_1"), lax.axis_index("pix")


def signal(sem, z, y, p):
    pl.semaphore_signal(sem, inc=1, device_id=(z, y, p), device_id_type=MESH)


def remote(src, dst, send, recv, z, y, p):
    return pltpu.make_async_remote_copy(
        src_ref=src, dst_ref=dst, send_sem=send, recv_sem=recv,
        device_id=(z, y, p), device_id_type=MESH,
    )


def coded(v):
    top = jnp.max(jnp.abs(v), axis=0, keepdims=True)
    e = jnp.clip(jnp.ceil(jnp.log2(jnp.maximum(top, 1e-38))), -126.0, 126.0)
    q = jnp.clip(jnp.round(v * jnp.exp2(-e) * 32767.0), -32767.0, 32767.0)
    return q.astype(jnp.int32).astype(jnp.int16), e


def lanes(i, n=LANES):
    return pl.ds(pl.multiple_of(i * n, n), n)


def kernel(
    days_ref, reflect_ref, cloud_ref, got_median, got_slope,
    day_in, xin, cin, send, part, mrow, recv, mrecv, tops,
    load_sem, own_sem, part_send, part_recv, data_send, data_recv,
    mean_send, mean_recv, relay_send, relay_recv, out_send, out_recv,
):
    z, y, p = place()
    me = z * SIDE + y
    early = z < HALF
    block = lax.rem(me, WORKERS)
    to_half = z - block // SIDE
    loads = [
        pltpu.make_async_copy(reflect_ref, xin, load_sem.at[0]),
        pltpu.make_async_copy(cloud_ref, cin, load_sem.at[1]),
        pltpu.make_async_copy(days_ref, day_in, load_sem.at[2]),
    ]
    barrier = pltpu.get_barrier_semaphore()
    shape = (BANDS, LANES)
    row = lax.broadcasted_iota(jnp.int32, shape, 0)
    lane = lax.broadcasted_iota(jnp.int32, shape, 1)

    def sized(some, sends, receives):
        return remote(some, some, sends, receives, z, y, p)

    @jax.named_scope("greet")
    def greet():
        for c in loads:
            c.start()
        for k in range(1, PEERS):
            signal(barrier, z, y, lax.rem(p + k, PEERS))

        @pl.when(early)
        def _():
            at_y = [lax.rem(y + k, SIDE) for k in range(SIDE)]

            def one(i, c):
                at_z = lax.rem(z + 2 + i, SIDE)
                for k in range(SIDE):

                    @pl.when((i != SIDE - 2) | (k != 0))
                    def _():
                        signal(barrier, at_z, at_y[k], p)

                return c

            lax.fori_loop(0, SIDE, one, 0)

    @jax.named_scope("load_wait")
    def load_wait():
        for c in loads:
            c.wait()

    @jax.named_scope("mark")
    def mark():
        def one(c, total):
            at = lanes(c)
            x = xin[:, at].astype(jnp.float32)
            clear = jnp.broadcast_to(cin[pl.ds(c, 1), :], shape) > 0
            send[:, at] = jnp.where(clear, x, sentinel).astype(jnp.bfloat16)
            return total + jnp.where(clear, x, 0.0)

        total = lax.fori_loop(0, CHUNKS, one, jnp.zeros(shape, jnp.float32), unroll=8)
        total = jnp.broadcast_to(jnp.sum(total, axis=1, keepdims=True), shape)
        clears = jnp.sum(cin[...].astype(jnp.float32), axis=0, keepdims=True)
        part[p, 0:1] = jnp.sum(jnp.where(row == lane, total, 0.0), axis=0, keepdims=True)
        part[p, 1:2] = jnp.broadcast_to(jnp.sum(clears, axis=1, keepdims=True), (1, LANES))

    @jax.named_scope("meet")
    def meet():
        @pl.when(early)
        def _():
            pl.semaphore_wait(barrier, PEERS - 1 + WORKERS - 1)

        @pl.when(jnp.logical_not(early))
        def _():
            pl.semaphore_wait(barrier, PEERS - 1 + WORKERS)

    def share(w):
        return send.at[:, lanes(w, WIDTH)]

    own = pltpu.make_async_copy(share(block), recv.at[me], own_sem)

    def to_workers(src, dst, sends, receives):
        for w in DEAL:

            @pl.when(me != w)
            def _():
                remote(src(w), dst.at[me], sends, receives, w // SIDE, w % SIDE, p).start()

    @jax.named_scope("deal")
    def deal():
        for k in range(1, PEERS):
            remote(part.at[p], part.at[p], part_send, part_recv, z, y, lax.rem(p + k, PEERS)).start()
        to_workers(share, recv, data_send, data_recv)

        @pl.when(early)
        def _():
            own.start()

    @jax.named_scope("pix_wait")
    def pix_wait():
        sized(part.at[pl.ds(0, PEERS - 1)], part_send, part_recv).wait_recv()

    @jax.named_scope("tell")
    def tell():
        sums = part[0]
        for k in range(1, PEERS):
            sums = sums + part[k]
        years = day_in[0, 0].astype(jnp.float32) * per_year
        at = lax.broadcasted_iota(jnp.int32, (1, LANES), 1)
        mrow[...] = jnp.where(at < BANDS, sums[0:1] / jnp.maximum(sums[1:2], 1.0), years)
        to_workers(lambda w: mrow, mrecv, mean_send, mean_recv)

    @jax.named_scope("data_wait")
    def data_wait():
        mrecv[me] = mrow[...]
        own.wait()
        sized(recv.at[pl.ds(0, DATES - 1)], data_send, data_recv).wait_recv()

    @jax.named_scope("medians")
    def medians():
        def one(i, c):
            at = lanes(i)
            count = jnp.zeros(shape, jnp.float32)
            xs = []
            for d in range(DATES):
                x = recv[d, :, at].astype(jnp.float32)
                count = count + jnp.where(x < 50.0, 1.0, 0.0)
                xs.append(x)
            for a, b, low, high in NETWORK:
                u, v = xs[a], xs[b]
                if low:
                    xs[a] = jnp.minimum(u, v)
                if high:
                    xs[b] = jnp.maximum(u, v)
            lower = jnp.floor((count - 1.0) * 0.5)
            upper = jnp.floor(count * 0.5)
            at_lower, at_upper = xs[0], xs[0]
            for k in range(1, KEPT):
                at_lower = jnp.where(lower == k, xs[k], at_lower)
                at_upper = jnp.where(upper == k, xs[k], at_upper)
            q, e = coded(0.5 * (at_lower + at_upper))
            got_median[block, :, at] = q
            tops[:, at] = e
            return c

        lax.fori_loop(0, WIDTH // LANES, one, 0)

    @jax.named_scope("mean_wait")
    def mean_wait():
        sized(mrecv.at[pl.ds(0, DATES - 1)], mean_send, mean_recv).wait_recv()

    @jax.named_scope("slopes")
    def slopes():
        told = mrecv[...].reshape(DATES, LANES).T
        means = told[:BANDS]
        times = told[8 : 8 + BANDS]
        zero = jnp.zeros(shape, jnp.float32)
        columns = range(WIDTH // LANES)
        state = [(zero,) * 5 for _ in columns]
        for d in range(DATES):
            mean = jnp.broadcast_to(means[:, d : d + 1], shape)
            t = jnp.broadcast_to(times[:, d : d + 1], shape)
            for i in columns:
                s0, s1, s2, sy, sty = state[i]
                x = recv[d, :, i * LANES : (i + 1) * LANES].astype(jnp.float32)
                clear = x < 50.0
                my = jnp.where(clear, x - mean, 0.0)
                mt = jnp.where(clear, t, 0.0)
                state[i] = (s0 + jnp.where(clear, 1.0, 0.0), s1 + mt, s2 + mt * t, sy + my, sty + my * t)
        for i in columns:
            s0, s1, s2, sy, sty = state[i]
            at = slice(i * LANES, (i + 1) * LANES)
            first = s0 + 1.0
            q, e = coded((first * sty - s1 * sy) / (first * (s2 + 1.0) - s1 * s1))
            ends = jnp.concatenate([e, tops[:, at]], axis=0).astype(jnp.int32).astype(jnp.int16)
            got_slope[block, 0:BANDS, at] = q
            got_slope[block, BANDS:8, at] = ends

    def relay(got, k):
        remote(got.at[block], got.at[block], relay_send.at[k], relay_recv.at[k], z + HALF, y, p).start()

    def spread(got, k):
        for w in ORDER:

            @pl.when(block != w)
            def _():
                remote(got.at[block], got.at[block], out_send.at[k], out_recv.at[k], to_half + w // SIDE, w % SIDE, p).start()

    greet()
    load_wait()
    mark()
    meet()
    deal()
    pix_wait()
    tell()
    outs = (got_median, got_slope)

    @pl.when(early)
    def _():
        data_wait()
        medians()
        with jax.named_scope("spread0"):
            relay(outs[0], 0)
            spread(outs[0], 0)
        mean_wait()
        slopes()
        with jax.named_scope("spread1"):
            relay(outs[1], 1)
            spread(outs[1], 1)

    @pl.when(jnp.logical_not(early))
    def _():
        for k, got in enumerate(outs):
            with jax.named_scope(f"relay{k}"):
                sized(got.at[block], relay_send.at[k], relay_recv.at[k]).wait_recv()
            with jax.named_scope(f"spread{k}"):
                spread(got, k)

    for k, got in enumerate(outs):
        with jax.named_scope(f"out_wait{k}"):
            sized(got.at[pl.ds(0, WORKERS - 1)], out_send.at[k], out_recv.at[k]).wait_recv()

    with jax.named_scope("drain"):
        sized(part.at[pl.ds(0, PEERS - 1)], part_send, part_recv).wait_send()

        def sent(n):
            sized(recv.at[pl.ds(0, n)], data_send, data_recv).wait_send()
            sized(mrecv.at[pl.ds(0, n)], mean_send, mean_recv).wait_send()

        @pl.when(early)
        def _():
            sent(WORKERS - 1)
            for k, got in enumerate(outs):
                sized(got.at[block], relay_send.at[k], relay_recv.at[k]).wait_send()

        @pl.when(jnp.logical_not(early))
        def _():
            sent(WORKERS)

        for k, got in enumerate(outs):
            sized(got.at[pl.ds(0, WORKERS - 1)], out_send.at[k], out_recv.at[k]).wait_send()


def finish(got_median, got_slope, median_ref, slope_ref):
    def one(w, c):
        at = lanes(w, WIDTH)
        slope = got_slope[w].astype(jnp.int32).astype(jnp.float32)
        scale = jnp.exp2(slope[BANDS:8]) * (1.0 / 32767.0)
        median_ref[:, at] = got_median[w].astype(jnp.int32).astype(jnp.float32) * scale[1:2]
        slope_ref[:, at] = slope[:BANDS] * scale[0:1]
        return c

    lax.fori_loop(0, WORKERS, one, 0, unroll=4)


def local(reflect, cloud_free, days):
    whole = pl.BlockSpec(memory_space=pltpu.VMEM)
    far = pl.BlockSpec(memory_space=pltpu.HBM)
    out = jax.ShapeDtypeStruct((BANDS, TILE), jnp.float32)
    dma = pltpu.SemaphoreType.DMA
    got = pl.pallas_call(
        kernel,
        out_shape=(
            jax.ShapeDtypeStruct((WORKERS, BANDS, WIDTH), jnp.int16),
            jax.ShapeDtypeStruct((WORKERS, 8, WIDTH), jnp.int16),
        ),
        in_specs=[far, far, far],
        out_specs=(whole, whole),
        scratch_shapes=[
            pltpu.SMEM((1, 1), jnp.int32),
            pltpu.VMEM((BANDS, TILE), jnp.bfloat16),
            pltpu.VMEM((CHUNKS, LANES), jnp.int32),
            pltpu.VMEM((BANDS, TILE), jnp.bfloat16),
            pltpu.VMEM((PEERS, 2, LANES), jnp.float32),
            pltpu.VMEM((1, LANES), jnp.float32),
            pltpu.VMEM((DATES, BANDS, WIDTH), jnp.bfloat16),
            pltpu.VMEM((DATES, 1, LANES), jnp.float32),
            pltpu.VMEM((1, WIDTH), jnp.float32),
            dma((3,)), dma, dma, dma, dma, dma, dma, dma,
            dma((2,)), dma((2,)), dma((2,)), dma((2,)),
        ],
        compiler_params=pltpu.CompilerParams(
            collective_id=0, has_side_effects=True, vmem_limit_bytes=8 * 2**20
        ),
    )(
        days.reshape(1, 1),
        *(
            pltpu.with_memory_space_constraint(a, pltpu.HBM)
            for a in (reflect.reshape(BANDS, TILE), cloud_free.reshape(CHUNKS, LANES))
        ),
    )
    return pl.pallas_call(
        finish, out_shape=(out, out), in_specs=[whole, whole], out_specs=(whole, whole),
        compiler_params=pltpu.CompilerParams(vmem_limit_bytes=4 * 2**20),
    )(*got)


def solution(mesh):
    torus = Mesh(mesh.devices.reshape(SIDE, SIDE, mesh.shape["pix"]), ("date_0", "date_1", "pix"))
    return jax.shard_map(
        local,
        mesh=torus,
        in_specs=(P(DATE, None, "pix"), P(DATE, "pix"), P(DATE)),
        out_specs=(P(None, "pix"), P(None, "pix")),
        check_vma=False,
    )
```

```python
import functools

import jax
import jax.numpy as jnp
from jax import lax
from jax.experimental import pallas as pl
from jax.experimental.pallas import tpu as pltpu
from jax.sharding import Mesh
from jax.sharding import PartitionSpec as P

MESH = pl.DeviceIdType.MESH
DATE = ("date_0", "date_1")
SIDE = 8
DATES = SIDE * SIDE
PEERS = 8
LANES = 128
TILE = 8192
WORKERS = 32
PLACE = [0, 1, 2, 3, 8, 9, 6, 7, 5, 10, 16, 4, 17, 11, 14, 15, 18, 24, 13, 12, 19, 23, 25, 22, 26, 21, 20, 31, 32, 30, 40, 48]
PARTNER = [50, 49, 58, 51, 56, 57, 54, 55, 61, 27, 45, 52, 44, 59, 62, 63, 35, 33, 53, 60, 43, 29, 41, 38, 34, 37, 36, 46, 39, 28, 42, 47]
WIDTH = TILE // WORKERS
CHUNKS = TILE // LANES
BANDS = 6
KEPT = DATES // 2 + 1
sentinel = 100.0
per_year = 1.0 / 365.0


def merged(lo, hi, r):
    step = 2 * r
    if step < hi - lo:
        yield from merged(lo, hi, step)
        yield from merged(lo + r, hi, step)
        yield from ((i, i + r) for i in range(lo + r, hi - r, step))
    else:
        yield (lo, lo + r)


def sorted_pairs(lo, hi):
    if hi > lo:
        mid = lo + (hi - lo) // 2
        yield from sorted_pairs(lo, mid)
        yield from sorted_pairs(mid + 1, hi)
        yield from merged(lo, hi, 1)


def pruned_network(n, kept):
    needed, steps = set(range(kept)), []
    for a, b in reversed(list(sorted_pairs(0, n - 1))):
        low, high = a in needed, b in needed
        if low or high:
            steps.append((a, b, low, high))
            needed |= {a, b}
    return steps[::-1]


LATE = [27, 29, 33, 41, 34, 28, 56, 50, 49, 35, 42, 39, 57, 38, 58, 43, 47, 51, 37, 46, 55, 36, 54, 45, 59, 63, 44, 53, 62, 52, 61, 60]
FIRST = 24
NETWORK = pruned_network(DATES, KEPT)


def place():
    return lax.axis_index("date_0"), lax.axis_index("date_1"), lax.axis_index("pix")


def signal(sem, z, y, p):
    pl.semaphore_signal(sem, inc=1, device_id=(z, y, p), device_id_type=MESH)


def remote(src, dst, send, recv, z, y, p):
    return pltpu.make_async_remote_copy(
        src_ref=src, dst_ref=dst, send_sem=send, recv_sem=recv,
        device_id=(z, y, p), device_id_type=MESH,
    )


def coded(v):
    top = jnp.max(jnp.abs(v), axis=0, keepdims=True)
    e = jnp.clip(jnp.ceil(jnp.log2(jnp.maximum(top, 1e-38))), -126.0, 126.0)
    q = jnp.clip(jnp.round(v * jnp.exp2(-e) * 32767.0), -32767.0, 32767.0)
    return q, e


def narrow(q):
    return q.astype(jnp.int32).astype(jnp.int16)


def split(ab, c):
    return [jnp.concatenate([ab[4 * i : 4 * i + 4], c[2 * i : 2 * i + 2]], axis=0) for i in range(2)]


def lanes(i, n=LANES):
    return pl.ds(pl.multiple_of(i * n, n), n)


def kernel(
    days_ref, reflect_ref, cloud_ref, got_median, got_slope,
    day_in, xin, cin, send, part, mrow, recv, mrecv, tops,
    load_sem, own_sem, part_send, part_recv, data_send, data_recv,
    mean_send, mean_recv, relay_send, relay_recv, out_send, out_recv,
):
    z, y, p = place()
    me = z * SIDE + y
    early = (z < 3) | ((z == 3) & ((y < 3) | (y > 5))) | ((y == 0) & (z < 7))
    block, pair = jnp.int32(0), jnp.int32(0)
    for w in range(1, WORKERS):
        block = jnp.where((me == PLACE[w]) | (me == PARTNER[w]), w, block)
    for w in range(WORKERS):
        pair = jnp.where(me == PLACE[w], PARTNER[w], pair)
    loads = [
        pltpu.make_async_copy(reflect_ref, xin, load_sem.at[0]),
        pltpu.make_async_copy(cloud_ref, cin, load_sem.at[1]),
        pltpu.make_async_copy(days_ref, day_in, load_sem.at[2]),
    ]
    barrier = pltpu.get_barrier_semaphore()
    shape = (BANDS, LANES)
    row = lax.broadcasted_iota(jnp.int32, shape, 0)
    lane = lax.broadcasted_iota(jnp.int32, shape, 1)
    band = jnp.where(lane < 4, lane, jnp.where(lane < 10, lane - 4, lane - 6))

    def sized(some, sends, receives):
        return remote(some, some, sends, receives, z, y, p)

    @jax.named_scope("greet")
    def greet():
        for c in loads:
            c.start()
        for k in range(1, PEERS):
            signal(barrier, z, y, lax.rem(p + k, PEERS))

        @pl.when(early)
        def _():
            at_y = [lax.rem(y + k, SIDE) for k in range(SIDE)]

            def one(i, c):
                at_z = lax.rem(z + 2 + i, SIDE)
                for k in range(SIDE):

                    @pl.when((i != SIDE - 2) | (k != 0))
                    def _():
                        signal(barrier, at_z, at_y[k], p)

                return c

            lax.fori_loop(0, SIDE, one, 0)

    @jax.named_scope("load_wait")
    def load_wait():
        for c in loads:
            c.wait()

    @jax.named_scope("mark")
    def mark():
        def one(w, total):
            for i in range(2):
                c = 2 * w + i
                x = xin[:, lanes(c)].astype(jnp.float32)
                clear = jnp.broadcast_to(cin[pl.ds(c, 1), :], shape) > 0
                marked = jnp.where(clear, x, sentinel).astype(jnp.bfloat16)
                send[w, i] = marked[:4]
                send[w, 2, 2 * i : 2 * i + 2] = marked[4:]
                total = total + jnp.where(clear, x, 0.0)
            return total

        total = lax.fori_loop(0, WORKERS, one, jnp.zeros(shape, jnp.float32), unroll=4)
        total = jnp.broadcast_to(jnp.sum(total, axis=1, keepdims=True), shape)
        clears = jnp.sum(cin[...].astype(jnp.float32), axis=0, keepdims=True)
        part[p, 0:1] = jnp.sum(jnp.where(row == band, total, 0.0), axis=0, keepdims=True)
        part[p, 1:2] = jnp.broadcast_to(jnp.sum(clears, axis=1, keepdims=True), (1, LANES))

    @jax.named_scope("meet")
    def meet():
        @pl.when(early)
        def _():
            pl.semaphore_wait(barrier, PEERS - 1 + WORKERS - 1)

        @pl.when(jnp.logical_not(early))
        def _():
            pl.semaphore_wait(barrier, PEERS - 1 + WORKERS)

    def share(w):
        return send.at[w]

    own = pltpu.make_async_copy(share(block), recv.at[me], own_sem)

    def to_workers(src, dst, sends, receives):
        for w in reversed(range(WORKERS)):

            @pl.when(me != PLACE[w])
            def _():
                remote(src(w), dst.at[me], sends, receives, PLACE[w] // SIDE, PLACE[w] % SIDE, p).start()

    @jax.named_scope("deal")
    def deal():
        for k in range(1, PEERS):
            remote(part.at[p], part.at[p], part_send, part_recv, z, y, lax.rem(p + k, PEERS)).start()
        to_workers(share, recv, data_send, data_recv)

        @pl.when(early)
        def _():
            own.start()

    @jax.named_scope("pix_wait")
    def pix_wait():
        sized(part.at[pl.ds(0, PEERS - 1)], part_send, part_recv).wait_recv()

    @jax.named_scope("tell")
    def tell():
        sums = part[0]
        for k in range(1, PEERS):
            sums = sums + part[k]
        years = day_in[0, 0].astype(jnp.float32) * per_year
        at = lax.broadcasted_iota(jnp.int32, (1, LANES), 1)
        mrow[...] = jnp.where(at < 12, sums[0:1] / jnp.maximum(sums[1:2], 1.0), years)
        to_workers(lambda w: mrow, mrecv, mean_send, mean_recv)

    @jax.named_scope("data_wait")
    def data_wait():
        mrecv[me] = mrow[...]
        own.wait()
        sized(recv.at[pl.ds(0, DATES - 1)], data_send, data_recv).wait_recv()

    def first_bands(d):
        return jnp.concatenate([recv[d, i].astype(jnp.float32) for i in range(2)], axis=0)

    def last_bands(d):
        return recv[d, 2].astype(jnp.float32)

    @jax.named_scope("medians")
    def medians():
        picked = []
        for piece in (first_bands, last_bands):
            count, xs = 0.0, []
            for d in range(DATES):
                x = piece(d)
                count = count + jnp.where(x < 50.0, 1.0, 0.0)
                xs.append(x)
            for a, b, low, high in NETWORK:
                u, v = xs[a], xs[b]
                if low:
                    xs[a] = jnp.minimum(u, v)
                if high:
                    xs[b] = jnp.maximum(u, v)
            lower = jnp.floor((count - 1.0) * 0.5)
            upper = jnp.floor(count * 0.5)
            at_lower, at_upper = xs[0], xs[0]
            for k in range(1, KEPT):
                at_lower = jnp.where(lower == k, xs[k], at_lower)
                at_upper = jnp.where(upper == k, xs[k], at_upper)
            picked.append(0.5 * (at_lower + at_upper))
        for i, v in enumerate(split(*picked)):
            q, e = coded(v)
            got_median[block, i] = narrow(q[:4])
            got_median[block, 2, 2 * i : 2 * i + 2] = narrow(q[4:])
            tops[:, i * LANES : (i + 1) * LANES] = e

    @jax.named_scope("mean_wait")
    def mean_wait():
        sized(mrecv.at[pl.ds(0, DATES - 1)], mean_send, mean_recv).wait_recv()

    @jax.named_scope("slopes")
    def slopes():
        told = mrecv[...].reshape(DATES, LANES).T
        made = []
        for piece, at, rows in ((first_bands, 0, 8), (last_bands, 8, 4)):
            s0 = s1 = s2 = sy = sty = jnp.zeros((rows, LANES), jnp.float32)
            for d in range(DATES):
                x = piece(d)
                mean = jnp.broadcast_to(told[at : at + rows, d : d + 1], x.shape)
                t = jnp.broadcast_to(told[16 : 16 + rows, d : d + 1], x.shape)
                clear = x < 50.0
                my = jnp.where(clear, x - mean, 0.0)
                mt = jnp.where(clear, t, 0.0)
                s0 = s0 + jnp.where(clear, 1.0, 0.0)
                s1 = s1 + mt
                s2 = s2 + mt * t
                sy = sy + my
                sty = sty + my * t
            first = s0 + 1.0
            made.append((first * sty - s1 * sy) / (first * (s2 + 1.0) - s1 * s1))
        for i, v in enumerate(split(*made)):
            q, e = coded(v)
            got_slope[block, i] = narrow(q[:4])
            got_slope[block, 2, 2 * i : 2 * i + 2] = narrow(q[4:])
            ends = jnp.concatenate([e, tops[:, i * LANES : (i + 1) * LANES]], axis=0)
            got_slope[block, 3, 2 * i : 2 * i + 2] = narrow(ends)

    def relay(got, k):
        remote(got.at[block], got.at[block], relay_send.at[k], relay_recv.at[k], pair // SIDE, lax.rem(pair, SIDE), p).start()

    def spread(got, k, group):
        for to in group:

            @pl.when(me != to)
            def _():
                remote(got.at[block], got.at[block], out_send.at[k], out_recv.at[k], to // SIDE, to % SIDE, p).start()

    greet()
    load_wait()
    mark()
    meet()
    deal()
    pix_wait()
    tell()
    outs = (got_median, got_slope)

    @pl.when(early)
    def _():
        data_wait()
        medians()
        with jax.named_scope("spread0"):
            relay(outs[0], 0)
            spread(outs[0], 0, PLACE[:FIRST])
        mean_wait()
        slopes()
        with jax.named_scope("spread1"):
            relay(outs[1], 1)
            spread(outs[1], 1, PLACE[:FIRST])
            spread(outs[0], 0, PLACE[FIRST:])
            spread(outs[1], 1, PLACE[FIRST:])

    @pl.when(jnp.logical_not(early))
    def _():
        for k, got in enumerate(outs):
            with jax.named_scope(f"relay{k}"):
                sized(got.at[block], relay_send.at[k], relay_recv.at[k]).wait_recv()
            with jax.named_scope(f"spread{k}"):
                spread(got, k, LATE)

    for k, got in enumerate(outs):
        with jax.named_scope(f"out_wait{k}"):
            sized(got.at[pl.ds(0, WORKERS - 1)], out_send.at[k], out_recv.at[k]).wait_recv()

    with jax.named_scope("drain"):
        sized(part.at[pl.ds(0, PEERS - 1)], part_send, part_recv).wait_send()

        def sent(n):
            sized(recv.at[pl.ds(0, n)], data_send, data_recv).wait_send()
            sized(mrecv.at[pl.ds(0, n)], mean_send, mean_recv).wait_send()

        @pl.when(early)
        def _():
            sent(WORKERS - 1)
            for k, got in enumerate(outs):
                sized(got.at[block], relay_send.at[k], relay_recv.at[k]).wait_send()

        @pl.when(jnp.logical_not(early))
        def _():
            sent(WORKERS)

        for k, got in enumerate(outs):
            sized(got.at[pl.ds(0, WORKERS - 1)], out_send.at[k], out_recv.at[k]).wait_send()


def finish(got_median, got_slope, median_ref, slope_ref):
    def one(w, c):
        scale = jnp.exp2(got_slope[w, 3].astype(jnp.int32).astype(jnp.float32)) * (1.0 / 32767.0)
        for k, (got, ref) in enumerate(((got_slope, slope_ref), (got_median, median_ref))):
            for i in range(2):
                at, by = lanes(2 * w + i), scale[2 * i + k : 2 * i + k + 1]
                some = slice(2 * i, 2 * i + 2)
                ref[:4, at] = got[w, i].astype(jnp.int32).astype(jnp.float32) * by
                ref[4:, at] = got[w, 2, some].astype(jnp.int32).astype(jnp.float32) * by
        return c

    lax.fori_loop(0, WORKERS, one, 0, unroll=4)


def local(reflect, cloud_free, days):
    whole = pl.BlockSpec(memory_space=pltpu.VMEM)
    far = pl.BlockSpec(memory_space=pltpu.HBM)
    out = jax.ShapeDtypeStruct((BANDS, TILE), jnp.float32)
    dma = pltpu.SemaphoreType.DMA
    got = pl.pallas_call(
        kernel,
        out_shape=(
            jax.ShapeDtypeStruct((WORKERS, 3, 4, LANES), jnp.int16),
            jax.ShapeDtypeStruct((WORKERS, 4, 4, LANES), jnp.int16),
        ),
        in_specs=[far, far, far],
        out_specs=(whole, whole),
        scratch_shapes=[
            pltpu.SMEM((1, 1), jnp.int32),
            pltpu.VMEM((BANDS, TILE), jnp.bfloat16),
            pltpu.VMEM((CHUNKS, LANES), jnp.int32),
            pltpu.VMEM((WORKERS, 3, 4, LANES), jnp.bfloat16),
            pltpu.VMEM((PEERS, 2, LANES), jnp.float32),
            pltpu.VMEM((1, LANES), jnp.float32),
            pltpu.VMEM((DATES, 3, 4, LANES), jnp.bfloat16),
            pltpu.VMEM((DATES, 1, LANES), jnp.float32),
            pltpu.VMEM((1, WIDTH), jnp.float32),
            dma((3,)), dma, dma, dma, dma, dma, dma, dma,
            dma((2,)), dma((2,)), dma((2,)), dma((2,)),
        ],
        compiler_params=pltpu.CompilerParams(
            collective_id=0, has_side_effects=True, vmem_limit_bytes=8 * 2**20
        ),
    )(
        days.reshape(1, 1),
        *(
            pltpu.with_memory_space_constraint(a, pltpu.HBM)
            for a in (reflect.reshape(BANDS, TILE), cloud_free.reshape(CHUNKS, LANES))
        ),
    )
    return pl.pallas_call(
        finish, out_shape=(out, out), in_specs=[whole, whole], out_specs=(whole, whole),
        compiler_params=pltpu.CompilerParams(vmem_limit_bytes=4 * 2**20),
    )(*got)


def solution(mesh):
    torus = Mesh(mesh.devices.reshape(SIDE, SIDE, mesh.shape["pix"]), ("date_0", "date_1", "pix"))
    return jax.shard_map(
        local,
        mesh=torus,
        in_specs=(P(DATE, None, "pix"), P(DATE, "pix"), P(DATE)),
        out_specs=(P(None, "pix"), P(None, "pix")),
        check_vma=False,
    )
```

```python
import functools

import jax
import jax.numpy as jnp
from jax import lax
from jax.experimental import pallas as pl
from jax.experimental.pallas import tpu as pltpu
from jax.sharding import Mesh
from jax.sharding import PartitionSpec as P

MESH = pl.DeviceIdType.MESH
DATE = ("date_0", "date_1")
SIDE = 8
DATES = SIDE * SIDE
PEERS = 8
LANES = 128
TILE = 8192
WORKERS = 32
PLACE = [0, 1, 2, 3, 8, 9, 6, 7, 5, 10, 16, 4, 17, 11, 14, 15, 18, 24, 13, 12, 19, 23, 25, 22, 26, 21, 20, 27, 31, 32, 30, 40]
PARTNER = [48, 49, 50, 51, 56, 57, 54, 55, 61, 58, 45, 52, 43, 59, 62, 63, 34, 41, 53, 60, 36, 39, 33, 38, 35, 37, 28, 44, 29, 47, 46, 42]
WIDTH = TILE // WORKERS
CHUNKS = TILE // LANES
BANDS = 6
KEPT = DATES // 2 + 1
sentinel = 100.0
per_year = 1.0 / 365.0


def merged(lo, hi, r):
    step = 2 * r
    if step < hi - lo:
        yield from merged(lo, hi, step)
        yield from merged(lo + r, hi, step)
        yield from ((i, i + r) for i in range(lo + r, hi - r, step))
    else:
        yield (lo, lo + r)


def sorted_pairs(lo, hi):
    if hi > lo:
        mid = lo + (hi - lo) // 2
        yield from sorted_pairs(lo, mid)
        yield from sorted_pairs(mid + 1, hi)
        yield from merged(lo, hi, 1)


def pruned_network(n, kept):
    needed, steps = set(range(kept)), []
    for a, b in reversed(list(sorted_pairs(0, n - 1))):
        low, high = a in needed, b in needed
        if low or high:
            steps.append((a, b, low, high))
            needed |= {a, b}
    return steps[::-1]


LATE = [48, 29, 33, 34, 41, 28, 56, 50, 49, 35, 42, 39, 57, 38, 58, 43, 47, 51, 37, 46, 55, 36, 54, 45, 59, 63, 44, 53, 62, 52, 61, 60]
FIRST = 24
NETWORK = pruned_network(DATES, KEPT)


def place():
    return lax.axis_index("date_0"), lax.axis_index("date_1"), lax.axis_index("pix")


def signal(sem, z, y, p):
    pl.semaphore_signal(sem, inc=1, device_id=(z, y, p), device_id_type=MESH)


def remote(src, dst, send, recv, z, y, p):
    return pltpu.make_async_remote_copy(
        src_ref=src, dst_ref=dst, send_sem=send, recv_sem=recv,
        device_id=(z, y, p), device_id_type=MESH,
    )


def coded(v):
    top = jnp.max(jnp.abs(v), axis=0, keepdims=True)
    e = jnp.clip(jnp.ceil(jnp.log2(jnp.maximum(top, 1e-38))), -126.0, 126.0)
    q = jnp.clip(jnp.round(v * jnp.exp2(-e) * 32767.0), -32767.0, 32767.0)
    return q, e


def narrow(q):
    return q.astype(jnp.int32).astype(jnp.int16)


def split(ab, c):
    return [jnp.concatenate([ab[4 * i : 4 * i + 4], c[2 * i : 2 * i + 2]], axis=0) for i in range(2)]


def lanes(i, n=LANES):
    return pl.ds(pl.multiple_of(i * n, n), n)


def kernel(
    days_ref, reflect_ref, cloud_ref, got_median, got_slope,
    day_in, xin, cin, send, part, mrow, recv, mrecv, tops,
    load_sem, own_sem, part_send, part_recv, data_send, data_recv,
    mean_send, mean_recv, relay_send, relay_recv, out_send, out_recv,
):
    z, y, p = place()
    me = z * SIDE + y
    early = (z < 3) | ((z == 3) & ((y < 4) | (y > 5))) | ((y == 0) & (z < 6))
    block, pair = jnp.int32(0), jnp.int32(0)
    for w in range(1, WORKERS):
        block = jnp.where((me == PLACE[w]) | (me == PARTNER[w]), w, block)
    for w in range(WORKERS):
        pair = jnp.where(me == PLACE[w], PARTNER[w], pair)
    loads = [
        pltpu.make_async_copy(reflect_ref, xin, load_sem.at[0]),
        pltpu.make_async_copy(cloud_ref, cin, load_sem.at[1]),
        pltpu.make_async_copy(days_ref, day_in, load_sem.at[2]),
    ]
    barrier = pltpu.get_barrier_semaphore()
    shape = (BANDS, LANES)
    row = lax.broadcasted_iota(jnp.int32, shape, 0)
    lane = lax.broadcasted_iota(jnp.int32, shape, 1)
    band = jnp.where(lane < 4, lane, jnp.where(lane < 10, lane - 4, lane - 6))

    def sized(some, sends, receives):
        return remote(some, some, sends, receives, z, y, p)

    @jax.named_scope("greet")
    def greet():
        for c in loads:
            c.start()
        for k in range(1, PEERS):
            signal(barrier, z, y, lax.rem(p + k, PEERS))

        @pl.when(early)
        def _():
            at_y = [lax.rem(y + k, SIDE) for k in range(SIDE)]

            def one(i, c):
                at_z = lax.rem(z + 2 + i, SIDE)
                for k in range(SIDE):

                    @pl.when((i != SIDE - 2) | (k != 0))
                    def _():
                        signal(barrier, at_z, at_y[k], p)

                return c

            lax.fori_loop(0, SIDE, one, 0)

    @jax.named_scope("load_wait")
    def load_wait():
        for c in loads:
            c.wait()

    @jax.named_scope("mark")
    def mark():
        def one(w, total):
            for i in range(2):
                c = 2 * w + i
                x = xin[:, lanes(c)].astype(jnp.float32)
                clear = jnp.broadcast_to(cin[pl.ds(c, 1), :], shape) > 0
                marked = jnp.where(clear, x, sentinel).astype(jnp.bfloat16)
                send[w, i] = marked[:4]
                send[w, 2, 2 * i : 2 * i + 2] = marked[4:]
                total = total + jnp.where(clear, x, 0.0)
            return total

        total = lax.fori_loop(0, WORKERS, one, jnp.zeros(shape, jnp.float32), unroll=4)
        total = jnp.broadcast_to(jnp.sum(total, axis=1, keepdims=True), shape)
        clears = jnp.sum(cin[...].astype(jnp.float32), axis=0, keepdims=True)
        part[p, 0:1] = jnp.sum(jnp.where(row == band, total, 0.0), axis=0, keepdims=True)
        part[p, 1:2] = jnp.broadcast_to(jnp.sum(clears, axis=1, keepdims=True), (1, LANES))

    @jax.named_scope("meet")
    def meet():
        @pl.when(early)
        def _():
            pl.semaphore_wait(barrier, PEERS - 1 + WORKERS - 1)

        @pl.when(jnp.logical_not(early))
        def _():
            pl.semaphore_wait(barrier, PEERS - 1 + WORKERS)

    def share(w):
        return send.at[w]

    own = pltpu.make_async_copy(share(block), recv.at[me], own_sem)

    def to_workers(src, dst, sends, receives):
        for w in reversed(range(WORKERS)):

            @pl.when(me != PLACE[w])
            def _():
                remote(src(w), dst.at[me], sends, receives, PLACE[w] // SIDE, PLACE[w] % SIDE, p).start()

    @jax.named_scope("deal")
    def deal():
        for k in range(1, PEERS):
            remote(part.at[p], part.at[p], part_send, part_recv, z, y, lax.rem(p + k, PEERS)).start()
        to_workers(share, recv, data_send, data_recv)

        @pl.when(early)
        def _():
            own.start()

    @jax.named_scope("pix_wait")
    def pix_wait():
        sized(part.at[pl.ds(0, PEERS - 1)], part_send, part_recv).wait_recv()

    @jax.named_scope("tell")
    def tell():
        sums = part[0]
        for k in range(1, PEERS):
            sums = sums + part[k]
        years = day_in[0, 0].astype(jnp.float32) * per_year
        at = lax.broadcasted_iota(jnp.int32, (1, LANES), 1)
        mrow[...] = jnp.where(at < 12, sums[0:1] / jnp.maximum(sums[1:2], 1.0), years)
        to_workers(lambda w: mrow, mrecv, mean_send, mean_recv)

    @jax.named_scope("data_wait")
    def data_wait():
        mrecv[me] = mrow[...]
        own.wait()
        sized(recv.at[pl.ds(0, DATES - 1)], data_send, data_recv).wait_recv()

    def first_bands(d):
        return jnp.concatenate([recv[d, i].astype(jnp.float32) for i in range(2)], axis=0)

    def last_bands(d):
        return recv[d, 2].astype(jnp.float32)

    @jax.named_scope("medians")
    def medians():
        picked = []
        for piece in (first_bands, last_bands):
            count, xs = 0.0, []
            for d in range(DATES):
                x = piece(d)
                count = count + jnp.where(x < 50.0, 1.0, 0.0)
                xs.append(x)
            for a, b, low, high in NETWORK:
                u, v = xs[a], xs[b]
                if low:
                    xs[a] = jnp.minimum(u, v)
                if high:
                    xs[b] = jnp.maximum(u, v)
            lower = jnp.floor((count - 1.0) * 0.5)
            upper = jnp.floor(count * 0.5)
            at_lower, at_upper = xs[0], xs[0]
            for k in range(1, KEPT):
                at_lower = jnp.where(lower == k, xs[k], at_lower)
                at_upper = jnp.where(upper == k, xs[k], at_upper)
            picked.append(0.5 * (at_lower + at_upper))
        for i, v in enumerate(split(*picked)):
            q, e = coded(v)
            got_median[block, i] = narrow(q[:4])
            got_median[block, 2, 2 * i : 2 * i + 2] = narrow(q[4:])
            tops[:, i * LANES : (i + 1) * LANES] = e

    @jax.named_scope("mean_wait")
    def mean_wait():
        sized(mrecv.at[pl.ds(0, DATES - 1)], mean_send, mean_recv).wait_recv()

    @jax.named_scope("slopes")
    def slopes():
        told = mrecv[...].reshape(DATES, LANES).T
        made = []
        for piece, at, rows in ((first_bands, 0, 8), (last_bands, 8, 4)):
            s0 = s1 = s2 = sy = sty = jnp.zeros((rows, LANES), jnp.float32)
            for d in range(DATES):
                x = piece(d)
                mean = jnp.broadcast_to(told[at : at + rows, d : d + 1], x.shape)
                t = jnp.broadcast_to(told[16 : 16 + rows, d : d + 1], x.shape)
                clear = x < 50.0
                my = jnp.where(clear, x - mean, 0.0)
                mt = jnp.where(clear, t, 0.0)
                s0 = s0 + jnp.where(clear, 1.0, 0.0)
                s1 = s1 + mt
                s2 = s2 + mt * t
                sy = sy + my
                sty = sty + my * t
            first = s0 + 1.0
            made.append((first * sty - s1 * sy) / (first * (s2 + 1.0) - s1 * s1))
        for i, v in enumerate(split(*made)):
            q, e = coded(v)
            got_slope[block, i] = narrow(q[:4])
            got_slope[block, 2, 2 * i : 2 * i + 2] = narrow(q[4:])
            ends = jnp.concatenate([e, tops[:, i * LANES : (i + 1) * LANES]], axis=0)
            got_slope[block, 3, 2 * i : 2 * i + 2] = narrow(ends)

    def relay(got, k):
        remote(got.at[block], got.at[block], relay_send.at[k], relay_recv.at[k], pair // SIDE, lax.rem(pair, SIDE), p).start()

    def spread(got, k, group):
        for to in group:

            @pl.when(me != to)
            def _():
                remote(got.at[block], got.at[block], out_send.at[k], out_recv.at[k], to // SIDE, to % SIDE, p).start()

    greet()
    load_wait()
    mark()
    meet()
    deal()
    pix_wait()
    tell()
    outs = (got_median, got_slope)

    @pl.when(early)
    def _():
        data_wait()
        medians()
        with jax.named_scope("spread0"):
            relay(outs[0], 0)
            spread(outs[0], 0, PLACE[:FIRST])
        mean_wait()
        slopes()
        with jax.named_scope("spread1"):
            relay(outs[1], 1)
            spread(outs[1], 1, PLACE[:FIRST])
            spread(outs[0], 0, PLACE[FIRST:])
            spread(outs[1], 1, PLACE[FIRST:])

    @pl.when(jnp.logical_not(early))
    def _():
        for k, got in enumerate(outs):
            with jax.named_scope(f"relay{k}"):
                sized(got.at[block], relay_send.at[k], relay_recv.at[k]).wait_recv()
            with jax.named_scope(f"spread{k}"):
                spread(got, k, LATE)

    for k, got in enumerate(outs):
        with jax.named_scope(f"out_wait{k}"):
            sized(got.at[pl.ds(0, WORKERS - 1)], out_send.at[k], out_recv.at[k]).wait_recv()

    with jax.named_scope("drain"):
        sized(part.at[pl.ds(0, PEERS - 1)], part_send, part_recv).wait_send()

        def sent(n):
            sized(recv.at[pl.ds(0, n)], data_send, data_recv).wait_send()
            sized(mrecv.at[pl.ds(0, n)], mean_send, mean_recv).wait_send()

        @pl.when(early)
        def _():
            sent(WORKERS - 1)
            for k, got in enumerate(outs):
                sized(got.at[block], relay_send.at[k], relay_recv.at[k]).wait_send()

        @pl.when(jnp.logical_not(early))
        def _():
            sent(WORKERS)

        for k, got in enumerate(outs):
            sized(got.at[pl.ds(0, WORKERS - 1)], out_send.at[k], out_recv.at[k]).wait_send()


def finish(got_median, got_slope, median_ref, slope_ref):
    def one(w, c):
        scale = jnp.exp2(got_slope[w, 3].astype(jnp.int32).astype(jnp.float32)) * (1.0 / 32767.0)
        for k, (got, ref) in enumerate(((got_slope, slope_ref), (got_median, median_ref))):
            for i in range(2):
                at, by = lanes(2 * w + i), scale[2 * i + k : 2 * i + k + 1]
                some = slice(2 * i, 2 * i + 2)
                ref[:4, at] = got[w, i].astype(jnp.int32).astype(jnp.float32) * by
                ref[4:, at] = got[w, 2, some].astype(jnp.int32).astype(jnp.float32) * by
        return c

    lax.fori_loop(0, WORKERS, one, 0, unroll=4)


def local(reflect, cloud_free, days):
    whole = pl.BlockSpec(memory_space=pltpu.VMEM)
    far = pl.BlockSpec(memory_space=pltpu.HBM)
    out = jax.ShapeDtypeStruct((BANDS, TILE), jnp.float32)
    dma = pltpu.SemaphoreType.DMA
    got = pl.pallas_call(
        kernel,
        out_shape=(
            jax.ShapeDtypeStruct((WORKERS, 3, 4, LANES), jnp.int16),
            jax.ShapeDtypeStruct((WORKERS, 4, 4, LANES), jnp.int16),
        ),
        in_specs=[far, far, far],
        out_specs=(whole, whole),
        scratch_shapes=[
            pltpu.SMEM((1, 1), jnp.int32),
            pltpu.VMEM((BANDS, TILE), jnp.bfloat16),
            pltpu.VMEM((CHUNKS, LANES), jnp.int32),
            pltpu.VMEM((WORKERS, 3, 4, LANES), jnp.bfloat16),
            pltpu.VMEM((PEERS, 2, LANES), jnp.float32),
            pltpu.VMEM((1, LANES), jnp.float32),
            pltpu.VMEM((DATES, 3, 4, LANES), jnp.bfloat16),
            pltpu.VMEM((DATES, 1, LANES), jnp.float32),
            pltpu.VMEM((1, WIDTH), jnp.float32),
            dma((3,)), dma, dma, dma, dma, dma, dma, dma,
            dma((2,)), dma((2,)), dma((2,)), dma((2,)),
        ],
        compiler_params=pltpu.CompilerParams(
            collective_id=0, has_side_effects=True, vmem_limit_bytes=8 * 2**20
        ),
    )(
        days.reshape(1, 1),
        *(
            pltpu.with_memory_space_constraint(a, pltpu.HBM)
            for a in (reflect.reshape(BANDS, TILE), cloud_free.reshape(CHUNKS, LANES))
        ),
    )
    return pl.pallas_call(
        finish, out_shape=(out, out), in_specs=[whole, whole], out_specs=(whole, whole),
        compiler_params=pltpu.CompilerParams(vmem_limit_bytes=4 * 2**20),
    )(*got)


def solution(mesh):
    torus = Mesh(mesh.devices.reshape(SIDE, SIDE, mesh.shape["pix"]), ("date_0", "date_1", "pix"))
    return jax.shard_map(
        local,
        mesh=torus,
        in_specs=(P(DATE, None, "pix"), P(DATE, "pix"), P(DATE)),
        out_specs=(P(None, "pix"), P(None, "pix")),
        check_vma=False,
    )
```

```python
import functools

import jax
import jax.numpy as jnp
from jax import lax
from jax.experimental import pallas as pl
from jax.experimental.pallas import tpu as pltpu
from jax.sharding import Mesh
from jax.sharding import PartitionSpec as P

MESH = pl.DeviceIdType.MESH
DATE = ("date_0", "date_1")
SIDE = 8
DATES = SIDE * SIDE
PEERS = 8
LANES = 128
TILE = 8192
WORKERS = 32
PLACE = [0, 1, 2, 3, 8, 9, 6, 7, 5, 10, 16, 4, 17, 11, 14, 15, 18, 24, 13, 12, 19, 23, 25, 22, 26, 21, 20, 27, 31, 32, 30, 40]
PARTNER = [48, 49, 50, 51, 56, 57, 54, 55, 61, 58, 45, 52, 43, 59, 62, 63, 34, 41, 53, 60, 36, 39, 33, 38, 35, 37, 28, 44, 29, 47, 46, 42]
WIDTH = TILE // WORKERS
CHUNKS = TILE // LANES
BANDS = 6
KEPT = DATES // 2 + 1
sentinel = 100.0
per_year = 1.0 / 365.0


def merged(lo, hi, r):
    step = 2 * r
    if step < hi - lo:
        yield from merged(lo, hi, step)
        yield from merged(lo + r, hi, step)
        yield from ((i, i + r) for i in range(lo + r, hi - r, step))
    else:
        yield (lo, lo + r)


def sorted_pairs(lo, hi):
    if hi > lo:
        mid = lo + (hi - lo) // 2
        yield from sorted_pairs(lo, mid)
        yield from sorted_pairs(mid + 1, hi)
        yield from merged(lo, hi, 1)


def pruned_network(n, kept):
    needed, steps = set(range(kept)), []
    for a, b in reversed(list(sorted_pairs(0, n - 1))):
        low, high = a in needed, b in needed
        if low or high:
            steps.append((a, b, low, high))
            needed |= {a, b}
    return steps[::-1]


LATE = [48, 29, 33, 34, 41, 28, 56, 50, 49, 35, 42, 39, 57, 38, 58, 43, 47, 51, 37, 46, 55, 36, 54, 45, 59, 63, 44, 53, 62, 52, 61, 60]
FIRST = 24
NETWORK = pruned_network(DATES, KEPT)


def place():
    return lax.axis_index("date_0"), lax.axis_index("date_1"), lax.axis_index("pix")


def signal(sem, z, y, p):
    pl.semaphore_signal(sem, inc=1, device_id=(z, y, p), device_id_type=MESH)


def remote(src, dst, send, recv, z, y, p):
    return pltpu.make_async_remote_copy(
        src_ref=src, dst_ref=dst, send_sem=send, recv_sem=recv,
        device_id=(z, y, p), device_id_type=MESH,
    )


def coded(v):
    top = jnp.max(jnp.abs(v), axis=0, keepdims=True)
    e = jnp.clip(jnp.ceil(jnp.log2(jnp.maximum(top, 1e-38))), -126.0, 126.0)
    q = jnp.clip(jnp.round(v * jnp.exp2(-e) * 32767.0), -32767.0, 32767.0)
    return q, e


def narrow(q):
    return q.astype(jnp.int32).astype(jnp.int16)


def split(ab, c):
    return [jnp.concatenate([ab[4 * i : 4 * i + 4], c[2 * i : 2 * i + 2]], axis=0) for i in range(2)]


def lanes(i, n=LANES):
    return pl.ds(pl.multiple_of(i * n, n), n)


def kernel(
    days_ref, reflect_ref, cloud_ref, got_median, got_slope,
    day_in, xin, cin, send, part, mrow, recv, mrecv, tops,
    load_sem, own_sem, part_send, part_recv, data_send, data_recv,
    mean_send, mean_recv, relay_send, relay_recv, out_send, out_recv,
):
    z, y, p = place()
    me = z * SIDE + y
    early = (z < 3) | ((z == 3) & ((y < 4) | (y > 5))) | ((y == 0) & (z < 6))
    block, pair = jnp.int32(0), jnp.int32(0)
    for w in range(1, WORKERS):
        block = jnp.where((me == PLACE[w]) | (me == PARTNER[w]), w, block)
    for w in range(WORKERS):
        pair = jnp.where(me == PLACE[w], PARTNER[w], pair)
    loads = [
        pltpu.make_async_copy(reflect_ref, xin, load_sem.at[0]),
        pltpu.make_async_copy(cloud_ref, cin, load_sem.at[1]),
        pltpu.make_async_copy(days_ref, day_in, load_sem.at[2]),
    ]
    barrier = pltpu.get_barrier_semaphore()
    shape = (BANDS, LANES)
    row = lax.broadcasted_iota(jnp.int32, shape, 0)
    lane = lax.broadcasted_iota(jnp.int32, shape, 1)
    band = jnp.where(lane < 4, lane, jnp.where(lane < 10, lane - 4, lane - 6))

    def sized(some, sends, receives):
        return remote(some, some, sends, receives, z, y, p)

    @jax.named_scope("greet")
    def greet():
        for c in loads:
            c.start()
        for k in range(1, PEERS):
            signal(barrier, z, y, lax.rem(p + k, PEERS))

        @pl.when(early)
        def _():
            at_y = [lax.rem(y + k, SIDE) for k in range(SIDE)]

            def one(i, c):
                at_z = lax.rem(z + 3 + i, SIDE)
                for k in range(SIDE):

                    @pl.when((i != SIDE - 3) | (k != 0))
                    def _():
                        signal(barrier, at_z, at_y[k], p)

                return c

            lax.fori_loop(0, SIDE, one, 0)

    @jax.named_scope("load_wait")
    def load_wait():
        for c in loads:
            c.wait()

    @jax.named_scope("mark")
    def mark():
        def one(w, total):
            for i in range(2):
                c = 2 * w + i
                x = xin[:, lanes(c)].astype(jnp.float32)
                clear = jnp.broadcast_to(cin[pl.ds(c, 1), :], shape) > 0
                marked = jnp.where(clear, x, sentinel).astype(jnp.bfloat16)
                send[w, i] = marked[:4]
                send[w, 2, 2 * i : 2 * i + 2] = marked[4:]
                total = total + jnp.where(clear, x, 0.0)
            return total

        total = lax.fori_loop(0, WORKERS, one, jnp.zeros(shape, jnp.float32), unroll=4)
        total = jnp.broadcast_to(jnp.sum(total, axis=1, keepdims=True), shape)
        clears = jnp.sum(cin[...].astype(jnp.float32), axis=0, keepdims=True)
        part[p, 0:1] = jnp.sum(jnp.where(row == band, total, 0.0), axis=0, keepdims=True)
        part[p, 1:2] = jnp.broadcast_to(jnp.sum(clears, axis=1, keepdims=True), (1, LANES))

    @jax.named_scope("meet")
    def meet():
        @pl.when(early)
        def _():
            pl.semaphore_wait(barrier, PEERS - 1 + WORKERS - 1)

        @pl.when(jnp.logical_not(early))
        def _():
            pl.semaphore_wait(barrier, PEERS - 1 + WORKERS)

    def share(w):
        return send.at[w]

    own = pltpu.make_async_copy(share(block), recv.at[me], own_sem)

    def to_workers(src, dst, sends, receives):
        for w in reversed(range(WORKERS)):

            @pl.when(me != PLACE[w])
            def _():
                remote(src(w), dst.at[me], sends, receives, PLACE[w] // SIDE, PLACE[w] % SIDE, p).start()

    @jax.named_scope("deal")
    def deal():
        for k in range(1, PEERS):
            remote(part.at[p], part.at[p], part_send, part_recv, z, y, lax.rem(p + k, PEERS)).start()
        to_workers(share, recv, data_send, data_recv)

        @pl.when(early)
        def _():
            own.start()

    @jax.named_scope("pix_wait")
    def pix_wait():
        sized(part.at[pl.ds(0, PEERS - 1)], part_send, part_recv).wait_recv()

    @jax.named_scope("tell")
    def tell():
        sums = part[0]
        for k in range(1, PEERS):
            sums = sums + part[k]
        years = day_in[0, 0].astype(jnp.float32) * per_year
        at = lax.broadcasted_iota(jnp.int32, (1, LANES), 1)
        mrow[...] = jnp.where(at < 12, sums[0:1] / jnp.maximum(sums[1:2], 1.0), years)
        to_workers(lambda w: mrow, mrecv, mean_send, mean_recv)

    @jax.named_scope("data_wait")
    def data_wait():
        mrecv[me] = mrow[...]
        own.wait()
        sized(recv.at[pl.ds(0, DATES - 1)], data_send, data_recv).wait_recv()

    def first_bands(d):
        return jnp.concatenate([recv[d, i].astype(jnp.float32) for i in range(2)], axis=0)

    def last_bands(d):
        return recv[d, 2].astype(jnp.float32)

    @jax.named_scope("medians")
    def medians():
        picked = []
        for piece in (first_bands, last_bands):
            count, xs = 0.0, []
            for d in range(DATES):
                x = piece(d)
                count = count + jnp.where(x < 50.0, 1.0, 0.0)
                xs.append(x)
            for a, b, low, high in NETWORK:
                u, v = xs[a], xs[b]
                if low:
                    xs[a] = jnp.minimum(u, v)
                if high:
                    xs[b] = jnp.maximum(u, v)
            lower = jnp.floor((count - 1.0) * 0.5)
            upper = jnp.floor(count * 0.5)
            at_lower, at_upper = xs[0], xs[0]
            for k in range(1, KEPT):
                at_lower = jnp.where(lower == k, xs[k], at_lower)
                at_upper = jnp.where(upper == k, xs[k], at_upper)
            picked.append(0.5 * (at_lower + at_upper))
        for i, v in enumerate(split(*picked)):
            q, e = coded(v)
            got_median[block, i] = narrow(q[:4])
            got_median[block, 2, 2 * i : 2 * i + 2] = narrow(q[4:])
            tops[:, i * LANES : (i + 1) * LANES] = e

    @jax.named_scope("mean_wait")
    def mean_wait():
        sized(mrecv.at[pl.ds(0, DATES - 1)], mean_send, mean_recv).wait_recv()

    @jax.named_scope("slopes")
    def slopes():
        told = mrecv[...].reshape(DATES, LANES).T
        pieces = ((first_bands, 0, 8), (last_bands, 8, 4))
        state = [(jnp.zeros((rows, LANES), jnp.float32),) * 5 for _, _, rows in pieces]
        for d in range(DATES):
            times = jnp.broadcast_to(told[16:24, d : d + 1], (8, LANES))
            for k, (piece, at, rows) in enumerate(pieces):
                s0, s1, s2, sy, sty = state[k]
                x, t = piece(d), times[:rows]
                mean = jnp.broadcast_to(told[at : at + rows, d : d + 1], x.shape)
                clear = x < 50.0
                my = jnp.where(clear, x - mean, 0.0)
                mt = jnp.where(clear, t, 0.0)
                state[k] = (s0 + jnp.where(clear, 1.0, 0.0), s1 + mt, s2 + mt * t, sy + my, sty + my * t)
        made = []
        for s0, s1, s2, sy, sty in state:
            first = s0 + 1.0
            made.append((first * sty - s1 * sy) / (first * (s2 + 1.0) - s1 * s1))
        for i, v in enumerate(split(*made)):
            q, e = coded(v)
            got_slope[block, i] = narrow(q[:4])
            got_slope[block, 2, 2 * i : 2 * i + 2] = narrow(q[4:])
            ends = jnp.concatenate([e, tops[:, i * LANES : (i + 1) * LANES]], axis=0)
            got_slope[block, 3, 2 * i : 2 * i + 2] = narrow(ends)

    def relay(got, k):
        remote(got.at[block], got.at[block], relay_send.at[k], relay_recv.at[k], pair // SIDE, lax.rem(pair, SIDE), p).start()

    def spread(got, k, group):
        for to in group:

            @pl.when(me != to)
            def _():
                remote(got.at[block], got.at[block], out_send.at[k], out_recv.at[k], to // SIDE, to % SIDE, p).start()

    greet()
    load_wait()
    mark()
    meet()
    deal()
    pix_wait()
    tell()
    outs = (got_median, got_slope)

    @pl.when(early)
    def _():
        data_wait()
        medians()
        with jax.named_scope("spread0"):
            relay(outs[0], 0)
            spread(outs[0], 0, PLACE[:FIRST])
        mean_wait()
        slopes()
        with jax.named_scope("spread1"):
            relay(outs[1], 1)
            spread(outs[1], 1, PLACE[:FIRST])
            spread(outs[0], 0, PLACE[FIRST:])
            spread(outs[1], 1, PLACE[FIRST:])

    @pl.when(jnp.logical_not(early))
    def _():
        for k, got in enumerate(outs):
            with jax.named_scope(f"relay{k}"):
                sized(got.at[block], relay_send.at[k], relay_recv.at[k]).wait_recv()
            with jax.named_scope(f"spread{k}"):
                spread(got, k, LATE)

    for k, got in enumerate(outs):
        with jax.named_scope(f"out_wait{k}"):
            sized(got.at[pl.ds(0, WORKERS - 1)], out_send.at[k], out_recv.at[k]).wait_recv()

    with jax.named_scope("drain"):
        sized(part.at[pl.ds(0, PEERS - 1)], part_send, part_recv).wait_send()

        def sent(n):
            sized(recv.at[pl.ds(0, n)], data_send, data_recv).wait_send()
            sized(mrecv.at[pl.ds(0, n)], mean_send, mean_recv).wait_send()

        @pl.when(early)
        def _():
            sent(WORKERS - 1)
            for k, got in enumerate(outs):
                sized(got.at[block], relay_send.at[k], relay_recv.at[k]).wait_send()

        @pl.when(jnp.logical_not(early))
        def _():
            sent(WORKERS)

        for k, got in enumerate(outs):
            sized(got.at[pl.ds(0, WORKERS - 1)], out_send.at[k], out_recv.at[k]).wait_send()


def finish(got_median, got_slope, median_ref, slope_ref):
    def one(w, c):
        scale = jnp.exp2(got_slope[w, 3].astype(jnp.int32).astype(jnp.float32)) * (1.0 / 32767.0)
        for k, (got, ref) in enumerate(((got_slope, slope_ref), (got_median, median_ref))):
            for i in range(2):
                at, by = lanes(2 * w + i), scale[2 * i + k : 2 * i + k + 1]
                some = slice(2 * i, 2 * i + 2)
                ref[:4, at] = got[w, i].astype(jnp.int32).astype(jnp.float32) * by
                ref[4:, at] = got[w, 2, some].astype(jnp.int32).astype(jnp.float32) * by
        return c

    lax.fori_loop(0, WORKERS, one, 0, unroll=4)


def local(reflect, cloud_free, days):
    whole = pl.BlockSpec(memory_space=pltpu.VMEM)
    far = pl.BlockSpec(memory_space=pltpu.HBM)
    out = jax.ShapeDtypeStruct((BANDS, TILE), jnp.float32)
    dma = pltpu.SemaphoreType.DMA
    got = pl.pallas_call(
        kernel,
        out_shape=(
            jax.ShapeDtypeStruct((WORKERS, 3, 4, LANES), jnp.int16),
            jax.ShapeDtypeStruct((WORKERS, 4, 4, LANES), jnp.int16),
        ),
        in_specs=[far, far, far],
        out_specs=(whole, whole),
        scratch_shapes=[
            pltpu.SMEM((1, 1), jnp.int32),
            pltpu.VMEM((BANDS, TILE), jnp.bfloat16),
            pltpu.VMEM((CHUNKS, LANES), jnp.int32),
            pltpu.VMEM((WORKERS, 3, 4, LANES), jnp.bfloat16),
            pltpu.VMEM((PEERS, 2, LANES), jnp.float32),
            pltpu.VMEM((1, LANES), jnp.float32),
            pltpu.VMEM((DATES, 3, 4, LANES), jnp.bfloat16),
            pltpu.VMEM((DATES, 1, LANES), jnp.float32),
            pltpu.VMEM((1, WIDTH), jnp.float32),
            dma((3,)), dma, dma, dma, dma, dma, dma, dma,
            dma((2,)), dma((2,)), dma((2,)), dma((2,)),
        ],
        compiler_params=pltpu.CompilerParams(
            collective_id=0, has_side_effects=True, vmem_limit_bytes=8 * 2**20
        ),
    )(
        days.reshape(1, 1),
        *(
            pltpu.with_memory_space_constraint(a, pltpu.HBM)
            for a in (reflect.reshape(BANDS, TILE), cloud_free.reshape(CHUNKS, LANES))
        ),
    )
    return pl.pallas_call(
        finish, out_shape=(out, out), in_specs=[whole, whole], out_specs=(whole, whole),
        compiler_params=pltpu.CompilerParams(vmem_limit_bytes=4 * 2**20),
    )(*got)


def solution(mesh):
    torus = Mesh(mesh.devices.reshape(SIDE, SIDE, mesh.shape["pix"]), ("date_0", "date_1", "pix"))
    return jax.shard_map(
        local,
        mesh=torus,
        in_specs=(P(DATE, None, "pix"), P(DATE, "pix"), P(DATE)),
        out_specs=(P(None, "pix"), P(None, "pix")),
        check_vma=False,
    )
```
